256 devices in a mesh: row: 8 (over z), col: 32 (over y, x, core).
Axes of the slice: x: 4, y: 4, z: 8, core: 2. Of those that a mesh axis runs over, the one named last changes fastest.
Arguments:
- node_latent: bfloat16 [262144, 128], P(('row', 'col')), may hold values from -6 to 6
- edge_latent: bfloat16 [1048576, 128], P(('row', 'col')), may hold values from -6 to 6
- senders: int32 [1048576], P(('row', 'col')), may hold values from 0 to 1535
- receivers: int32 [1048576], P(('row', 'col')), may hold values from 0 to 1023
- send_index: int32 [256, 4, 128], P(('row', 'col')), may hold values from 0 to 1023
- context_table: bfloat16 [2048, 128], P(('row', 'col')), may hold values from -6 to 6
- region: int32 [262144], P(('row', 'col')), may hold values from 0 to 2047
- edge_w1: bfloat16 [2, 384, 128], replicated, may hold values from -0.3125 to 0.3125
- edge_w2: bfloat16 [2, 128, 128], replicated, may hold values from -0.5 to 0.5
- edge_bias: float32 [2, 3, 128], replicated, may hold values from -3 to 3
- edge_gain: float32 [2, 128], replicated, may hold values from 0.25 to 1.75
- node_w1: bfloat16 [2, 384, 128], replicated, may hold values from -0.3125 to 0.3125
- node_wg: bfloat16 [2, 128, 128], replicated, may hold values from -0.5 to 0.5
- node_w2: bfloat16 [2, 128, 128], replicated, may hold values from -0.5 to 0.5
- node_bias: float32 [2, 3, 128], replicated, may hold values from -3 to 3
- node_gain: float32 [2, 128], replicated, may hold values from 0.25 to 1.75
Outputs:
- node_out: bfloat16 [262144, 128], P(('row', 'col'))
- edge_out: bfloat16 [1048576, 128], P(('row', 'col'))
The draws below stay inside these ranges and needn't reach their ends.
Inputs may be any that keep to these rules, and one draw needn't show every extreme that they name: senders index the extended table of the edge's own partition: below 1024 its own nodes, then the four received blocks of 128 rows in the order above, below, left, right. receivers are nodes of the edge's own partition. `send_index`: rows of the sending partition's own nodes; repeats may occur.
All inputs are finite; a program needn't handle non-finite values.
Results may differ from the reference program's by a relative error of at most 0.0085.
Values may be sent and summed in bfloat16 or wider, within the bound.
No kernel may reach another device: no remote copies, remote signals or barrier semaphores. Data moves between devices by JAX's collectives and lax.ppermute only.
A program may use at most 64 MiB of HBM per device.

```python
import math
import jax
import jax.numpy as jnp
from jax import lax

LATENT = 128
NODES_DEV = 1024
BOUNDARY = 128
LAYERS = 2
EDGES_DEV = 4096
EXTENDED = 1536
PARTS_SIZE = 256
NODES = 262144
EDGES = 1048576
REGIONS = 2048
N_ROW = 8
N_COL = 32


def with_ends(values, key, low, high):
    shape = values.shape
    index_at = [jax.random.randint(jax.random.fold_in(key, axis), (), 0, shape[axis]) for axis in range(len(shape))]
    values = values.at[tuple(index_at)].set(low)
    longest = shape.index(max(shape))
    index_at[longest] = (index_at[longest] + 1) % shape[longest]
    return values.at[tuple(index_at)].set(high)


def steps_of(stream_key, extent, cuts, least, top_value):
    factor_of = 1.0
    for position, shards_of in cuts:
        steps = jax.random.uniform(jax.random.fold_in(jax.random.fold_in(stream_key, 6), position), (shards_of,), jnp.float32, least / len(cuts), top_value / len(cuts))
        factor_of = factor_of * jnp.repeat(jnp.exp(steps), extent[position] // shards_of).reshape((-1,) + (1,) * (len(extent) - 1 - position))
    return factor_of


def bell_draw(stream_key, dims, deviation, reach, cuts=(), dtype=jnp.bfloat16):
    level = steps_of(stream_key, dims, cuts, -0.22, 0.18) if cuts else 1.0
    drawn = jax.random.normal(stream_key, dims, jnp.float32) * deviation * level
    return jnp.minimum(jnp.maximum(drawn, -reach), reach).astype(dtype)


def setup_inputs(seed: int = 0) -> dict:
    splits = jax.random.split(jax.random.key(seed), 17)
    node_latent = bell_draw(splits[0], (NODES, LATENT), 1.0, 6.0, ((0, 256),))
    edge_latent = bell_draw(splits[1], (EDGES, LATENT), 1.0, 6.0, ((0, 256),))
    senders = with_ends(jax.random.randint(splits[2], (EDGES,), 0, EXTENDED), jax.random.fold_in(splits[2], 1), 0, EXTENDED - 1).astype(jnp.int32)
    receivers = with_ends(jax.random.randint(splits[3], (EDGES,), 0, NODES_DEV), jax.random.fold_in(splits[3], 1), 0, NODES_DEV - 1).astype(jnp.int32)
    send_index = with_ends(jax.random.randint(splits[4], (PARTS_SIZE, 4, BOUNDARY), 0, NODES_DEV), jax.random.fold_in(splits[4], 1), 0, NODES_DEV - 1).astype(jnp.int32)
    context_table = bell_draw(splits[5], (REGIONS, LATENT), 1.0, 6.0, ((0, 256),))
    region = with_ends(jax.random.randint(splits[6], (NODES,), 0, REGIONS), jax.random.fold_in(splits[6], 1), 0, REGIONS - 1).astype(jnp.int32)
    edge_w1 = bell_draw(splits[7], (LAYERS, 3 * LATENT, LATENT), (3 * LATENT) ** -0.5, 0.3125)
    edge_w2 = bell_draw(splits[8], (LAYERS, LATENT, LATENT), LATENT ** -0.5, 0.5)
    edge_bias = bell_draw(splits[9], (LAYERS, 3, LATENT), 0.5, 3.0, (), jnp.float32)
    edge_gain = jnp.clip(1.0 + 0.15 * jax.random.normal(splits[10], (LAYERS, LATENT), jnp.float32), 0.25, 1.75)
    node_w1 = bell_draw(splits[11], (LAYERS, 3 * LATENT, LATENT), (3 * LATENT) ** -0.5, 0.3125)
    node_wg = bell_draw(splits[12], (LAYERS, LATENT, LATENT), LATENT ** -0.5, 0.5)
    node_w2 = bell_draw(splits[13], (LAYERS, LATENT, LATENT), LATENT ** -0.5, 0.5)
    node_bias = bell_draw(splits[14], (LAYERS, 3, LATENT), 0.5, 3.0, (), jnp.float32)
    node_gain = jnp.clip(1.0 + 0.15 * jax.random.normal(splits[15], (LAYERS, LATENT), jnp.float32), 0.25, 1.75)
    return dict(node_latent=node_latent, edge_latent=edge_latent, senders=senders, receivers=receivers, send_index=send_index, context_table=context_table, region=region, edge_w1=edge_w1, edge_w2=edge_w2, edge_bias=edge_bias, edge_gain=edge_gain, node_w1=node_w1, node_wg=node_wg, node_w2=node_w2, node_bias=node_bias, node_gain=node_gain)


EPS = 1e-05

def norm_tail(pre, w_out, b_out, gain, shift):
    hidden = jax.nn.relu(pre).astype(jnp.bfloat16)
    y_val = jnp.dot(hidden, w_out, preferred_element_type=jnp.float32) + b_out
    centred = y_val - lax.optimization_barrier(jnp.mean(y_val, axis=-1, keepdims=True))
    spread = lax.optimization_barrier(jnp.mean(centred * centred, axis=-1, keepdims=True))
    return centred * lax.rsqrt(spread + EPS) * gain + shift

def edge_step(extended, edges, senders, receivers, w_in, w_out, bias, gain):
    feats = jnp.concatenate([jnp.take(extended, senders, axis=0), jnp.take(extended, receivers, axis=0), edges], axis=1)
    pre = jnp.dot(feats, w_in, preferred_element_type=jnp.float32) + bias[0]
    return (edges.astype(jnp.float32) + norm_tail(pre, w_out, bias[1], gain, bias[2])).astype(jnp.bfloat16)

def node_step(nodes, new_edges, receivers, context_rows, w_in, w_out, bias, gain, shift_in):
    summed = jax.ops.segment_sum(new_edges.astype(jnp.float32), receivers, num_segments=nodes.shape[0]).astype(jnp.bfloat16)
    feats = jnp.concatenate([nodes, summed, context_rows], axis=1)
    pre = jnp.dot(feats, w_in, preferred_element_type=jnp.float32) + shift_in
    return (nodes.astype(jnp.float32) + norm_tail(pre, w_out, bias[1], gain, bias[2])).astype(jnp.bfloat16)

def pick_rows(nodes, index):
    width = nodes.shape[1]
    return jnp.take(nodes, index.reshape(-1), axis=0).reshape(4, index.shape[1], width)

def with_halo(nodes, send_index):
    sent = jax.vmap(jax.vmap(pick_rows))(nodes, send_index)
    zero_row = jnp.zeros_like(sent[:1, :, 0])
    from_above = jnp.concatenate([zero_row, sent[:-1, :, 0]], axis=0)
    from_below = jnp.concatenate([sent[1:, :, 1], zero_row], axis=0)
    zero_col = jnp.zeros_like(sent[:, :1, 2])
    from_left = jnp.concatenate([zero_col, sent[:, :-1, 2]], axis=1)
    from_right = jnp.concatenate([sent[:, 1:, 3], zero_col], axis=1)
    return jnp.concatenate([nodes, from_above, from_below, from_left, from_right], axis=2)

def reference(node_latent, edge_latent, senders, receivers, send_index, context_table, region, edge_w1, edge_w2, edge_bias, edge_gain, node_w1, node_wg, node_w2, node_bias, node_gain):
    width = node_latent.shape[1]
    pooled = lax.optimization_barrier(jnp.sum(node_latent.astype(jnp.float32), axis=0)) / math.sqrt(NODES)
    nodes = node_latent.reshape(N_ROW, N_COL, NODES_DEV, width)
    edges = edge_latent.reshape(PARTS_SIZE, EDGES_DEV, width)
    sender_rows = senders.reshape(PARTS_SIZE, EDGES_DEV)
    receiver_rows = receivers.reshape(PARTS_SIZE, EDGES_DEV)
    index = send_index.reshape(N_ROW, N_COL, 4, BOUNDARY)
    context_rows = jnp.take(context_table, region, axis=0).reshape(PARTS_SIZE, NODES_DEV, width)
    for layer in range(LAYERS):
        extended = with_halo(nodes, index).reshape(PARTS_SIZE, EXTENDED, width)
        flat = nodes.reshape(PARTS_SIZE, NODES_DEV, width)
        shift_in = node_bias[layer, 0] + jnp.dot(pooled, node_wg[layer].astype(jnp.float32), precision=lax.Precision.HIGHEST)

        def one_part(items, layer=layer, shift_in=shift_in):
            ext_p, edges_p, send_p, recv_p, nodes_p, ctx_p = items
            new_edges = edge_step(ext_p, edges_p, send_p, recv_p, edge_w1[layer], edge_w2[layer], edge_bias[layer], edge_gain[layer])
            new_nodes = node_step(nodes_p, new_edges, recv_p, ctx_p, node_w1[layer], node_w2[layer], node_bias[layer], node_gain[layer], shift_in)
            return (new_edges, new_nodes)
        edges, flat = lax.map(one_part, (extended, edges, sender_rows, receiver_rows, flat, context_rows))
        nodes = flat.reshape(N_ROW, N_COL, NODES_DEV, width)
    return (nodes.reshape(NODES, width), edges.reshape(EDGES, width))
```

```python
import functools
import math

import jax
import jax.numpy as jnp
from jax import lax
from jax.experimental import pallas as pl
from jax.experimental.pallas import tpu as pltpu
from jax.sharding import Mesh
from jax.sharding import PartitionSpec as P

LAYERS = 2
COL = ("col_0", "col_1", "col_2")
ROW_COL = ("row", "col_0", "col_1", "col_2")
EPS = 1e-05
W = 128
TILE = 512
BF = jnp.bfloat16
F32 = jnp.float32
VM = pltpu.VMEM


def dot(a, b):
    return jnp.dot(a, b, preferred_element_type=F32)


def columns(stack, count):
    turned = jnp.transpose(stack)
    return [
        jnp.broadcast_to(turned[:, k : k + 1], (W, W)).astype(jnp.int16) for k in range(count)
    ]


def column_hot(col, count):
    lane = lax.broadcasted_iota(jnp.int16, (1, W), 1)
    one, zero = jnp.ones((), BF), jnp.zeros((), BF)
    pieces = [
        jnp.where(col == lane + jnp.int16(W * c), one, zero) for c in range(count // W)
    ]
    return jnp.concatenate(pieces, axis=1)


def row_hot(row, count):
    spread = jnp.broadcast_to(row, (16, W)).astype(jnp.int16)
    at = lax.broadcasted_iota(jnp.int16, (16, W), 0)
    one, zero = jnp.ones((), BF), jnp.zeros((), BF)
    pieces = [jnp.where(spread == at + jnp.int16(16 * c), one, zero) for c in range(count // 16)]
    return jnp.concatenate(pieces, axis=0)


def split2(value):
    high = value.astype(BF)
    low = (value - high.astype(F32)).astype(BF)
    return high, low


def split3(value):
    high = value.astype(BF)
    rest = value - high.astype(F32)
    mid = rest.astype(BF)
    low = (rest - mid.astype(F32)).astype(BF)
    return high, mid, low


def centred_weights(w_out, b_out):
    full = w_out.astype(F32)
    full = full - jnp.mean(full, axis=1, keepdims=True)
    high, low = split2(full)
    return jnp.concatenate([high, low], axis=1), b_out - jnp.mean(b_out, axis=1, keepdims=True)


def norm_tail(pre, w_two, b_centred, gain, shift):
    hidden = jnp.maximum(pre, 0.0).astype(BF)
    both = dot(hidden, w_two)
    centred = both[:, :W] + both[:, W:] + b_centred
    averager = jnp.full((W, W), 1.0 / W, BF)
    spread = dot((centred * centred).astype(BF), averager)
    return centred * lax.rsqrt(spread + EPS) * gain + shift


def picked_rows(table_two, half_rows, stack, count):
    cols = columns(stack, count)
    col = jnp.concatenate(cols, axis=0)
    hot = column_hot(col & jnp.int16(half_rows - 1), half_rows)
    both = dot(hot, table_two)
    upper = col.astype(jnp.int32) >= half_rows
    return jnp.where(upper, both[:, W:], both[:, :W]).astype(BF)


def phases(first, second, odd):
    return jnp.where(odd, second, first), jnp.where(odd, first, second)


def send_rows(table_two, half_rows, send_ref):
    row_odd = lax.rem(lax.axis_index("row"), 2) == 1
    col_odd = lax.axis_index("col_2") == 1
    index = [send_ref[0, k : k + 1, :] for k in range(4)]
    index_a, index_b = phases(index[0], index[1], row_odd)
    index_c, index_d = phases(index[2], index[3], col_odd)
    stack = jnp.concatenate([index_a, index_b, index_c, index_d] + [index_a] * 4, axis=0)
    return picked_rows(table_two, half_rows, stack, 4)


def start_kernel(nodes_ref, send_ref, context_ref, payload_ref, *picked_refs):
    nodes = nodes_ref[...]
    half = nodes.shape[0] // 2
    two = jnp.concatenate([nodes[:half], nodes[half:]], axis=1)
    picked = send_rows(two, half, send_ref)
    for k, ref in enumerate(picked_refs):
        ref[...] = picked[W * k : W * (k + 1)]
    local_sum = jnp.sum(nodes.astype(F32), axis=0, keepdims=True)
    high, mid, low = split3(local_sum)
    block = jnp.concatenate(
        [
            context_ref[...].astype(F32),
            high.astype(F32),
            mid.astype(F32),
            low.astype(F32),
            jnp.zeros((5, W), F32),
        ],
        axis=0,
    ).astype(BF)
    for k in range(payload_ref.shape[0]):
        payload_ref[k] = block


def middle_kernel(got_ref, payload_ref):
    got = [got_ref[k].astype(F32) for k in range(got_ref.shape[0])]
    total = functools.reduce(
        lambda a, b: a + b, [g[8:9] + (g[9:10] + g[10:11]) for g in got]
    )
    high, mid, low = split3(total)
    block = jnp.concatenate(
        [g[:8] for g in got]
        + [high.astype(F32), mid.astype(F32), low.astype(F32), jnp.zeros((13, W), F32)],
        axis=0,
    ).astype(BF)
    for k in range(payload_ref.shape[0]):
        payload_ref[k] = block


def edge_kernel(
    layer,
    nodes_ref,
    halo_a,
    halo_b,
    halo_c,
    halo_d,
    senders_ref,
    receivers_ref,
    edges_ref,
    w_in_ref,
    w_out_ref,
    bias_ref,
    gain_ref,
    fresh_ref,
    summed_ref,
    send_table,
    recv_table,
    send_col,
    recv_col,
    acc,
    w_two,
):
    step = pl.program_id(0)
    node_count = nodes_ref.shape[0]
    extent = node_count + 4 * W
    send_half = extent // 2
    recv_half = node_count // 2

    @pl.when(step == 0)
    def _():
        nodes = nodes_ref[...]
        ext = jnp.concatenate(
            [nodes, halo_a[...], halo_b[...], halo_c[...], halo_d[...]], axis=0
        )
        from_send = dot(ext, w_in_ref[0, :W]).astype(BF)
        from_recv = dot(nodes, w_in_ref[0, W : 2 * W]).astype(BF)
        send_table[:send_half, :W] = from_send[:send_half]
        send_table[:send_half, W:] = from_send[send_half:]
        send_table[send_half:, :W] = w_in_ref[0, 2 * W :]
        send_table[send_half:, W:] = w_in_ref[0, 2 * W :]
        recv_table[:, :W] = from_recv[:recv_half]
        recv_table[:, W:] = from_recv[recv_half:]
        w_two[...] = centred_weights(w_out_ref[0], bias_ref[0, 1:2])[0]
        senders = senders_ref[...]
        row_flip = jnp.where(lax.rem(lax.axis_index("row"), 2) == 1, 0, W)
        col_flip = jnp.where(lax.axis_index("col_2") == 1, 0, W)
        flip = jnp.where(senders < node_count + 2 * W, row_flip, col_flip)
        senders = jnp.where(senders < node_count, senders, senders ^ flip)
        receivers = receivers_ref[...]
        for values, ref in ((senders, send_col), (receivers, recv_col)):
            count = values.shape[0]
            for k, block in enumerate(columns(values, count)):
                ref[W * k : W * (k + 1)] = block
        acc[...] = jnp.zeros_like(acc)

    at = pl.ds(pl.multiple_of(step * TILE, TILE), TILE)
    edges = edges_ref[...]
    send16 = send_col[at]
    recv16 = recv_col[at]
    send_local = jnp.where(send16 >= jnp.int16(send_half), send16 - jnp.int16(send_half), send16)
    send_hot = column_hot(send_local, send_half)
    recv_hot = column_hot(recv16 & jnp.int16(recv_half - 1), recv_half)
    both_s = dot(jnp.concatenate([send_hot, edges], axis=1), send_table[...])
    both_r = dot(recv_hot, recv_table[...])
    upper_s = send16.astype(jnp.int32) >= send_half
    upper_r = recv16.astype(jnp.int32) >= recv_half
    pre = (
        jnp.where(upper_s, both_s[:, W:], both_s[:, :W])
        + jnp.where(upper_r, both_r[:, W:], both_r[:, :W])
        + bias_ref[0, 0:1]
    )
    b_out = bias_ref[0, 1:2]
    b_centred = b_out - jnp.mean(b_out, axis=1, keepdims=True)
    tail = norm_tail(
        pre, w_two[...], b_centred, gain_ref[layer : layer + 1], bias_ref[0, 2:3]
    )
    fresh = (edges.astype(F32) + tail).astype(BF)
    fresh_ref[...] = fresh
    lower16 = recv16 < jnp.int16(recv_half)
    zero = jnp.zeros((), BF)
    fresh_two = jnp.concatenate(
        [jnp.where(lower16, fresh, zero), jnp.where(lower16, zero, fresh)], axis=1
    )
    per = TILE // W
    rows = receivers_ref[pl.ds(step * per, per)] & (recv_half - 1)
    turned = jnp.concatenate(
        [row_hot(rows[k : k + 1], recv_half) for k in range(per)], axis=1
    )
    acc[...] += dot(turned, fresh_two)

    @pl.when(step == pl.num_programs(0) - 1)
    def _():
        summed_ref[:recv_half] = acc[:, :W].astype(BF)
        summed_ref[recv_half:] = acc[:, W:].astype(BF)


def whole(shape):
    return pl.BlockSpec(shape, lambda i: (0,) * len(shape))


def of_layer(shape, layer):
    return pl.BlockSpec((1, *shape[1:]), lambda i: (layer,) + (0,) * (len(shape) - 1))


def edge_step(layer, nodes, halo, senders, receivers, edges, w_in, w_out, bias, gain):
    node_count, edge_count = nodes.shape[0], edges.shape[0]
    half, ext_half = node_count // 2, (node_count + 4 * W) // 2
    steps = edge_count // TILE
    flops = 2 * edge_count * W * (2 * ext_half + 4 * half + 8 * W)
    return pl.pallas_call(
        functools.partial(edge_kernel, layer),
        grid=(steps,),
        in_specs=[
            whole(nodes.shape),
            *[whole((W, W))] * 4,
            whole(senders.shape),
            whole(receivers.shape),
            pl.BlockSpec((TILE, W), lambda i: (i, 0)),
            of_layer(w_in.shape, layer),
            of_layer(w_out.shape, layer),
            of_layer(bias.shape, layer),
            whole(gain.shape),
        ],
        out_specs=[pl.BlockSpec((TILE, W), lambda i: (i, 0)), whole(nodes.shape)],
        out_shape=[
            jax.ShapeDtypeStruct(edges.shape, BF),
            jax.ShapeDtypeStruct(nodes.shape, BF),
        ],
        scratch_shapes=[
            VM((ext_half + W, 2 * W), BF),
            VM((half, 2 * W), BF),
            VM((edge_count, W), jnp.int16),
            VM((edge_count, W), jnp.int16),
            VM((half, 2 * W), F32),
            VM((W, 2 * W), BF),
        ],
        compiler_params=pltpu.CompilerParams(dimension_semantics=("arbitrary",)),
        cost_estimate=pl.CostEstimate(
            flops=flops, bytes_accessed=4 * edge_count * W, transcendentals=0
        ),
        name=f"edges_{layer}",
    )(nodes, *halo, senders, receivers, edges, w_in, w_out, bias, gain)


def node_update(layer, nodes, summed, context, pooled, w_in_ref, wg_ref, w_out_ref, bias_ref, gain_ref):
    parts = jnp.concatenate(
        [p.astype(F32) for p in split3(pooled)] + [jnp.zeros((13, W), F32)], axis=0
    ).astype(BF)
    through = dot(parts, wg_ref[0])
    shift_in = bias_ref[0, 0:1] + (through[0:1] + (through[1:2] + through[2:3]))
    w_two, b_centred = centred_weights(w_out_ref[0], bias_ref[0, 1:2])
    feats = jnp.concatenate([nodes, summed, context], axis=1)
    pre = dot(feats, w_in_ref[0]) + shift_in
    tail = norm_tail(pre, w_two, b_centred, gain_ref[layer : layer + 1], bias_ref[0, 2:3])
    return (nodes.astype(F32) + tail).astype(BF)


def first_node_kernel(
    nodes_ref,
    summed_ref,
    table_ref,
    region_ref,
    send_ref,
    w_in_ref,
    wg_ref,
    w_out_ref,
    bias_ref,
    gain_ref,
    nodes_out,
    context_out,
    pooled_out,
    a_out,
    b_out,
    c_out,
    d_out,
    table_two,
    fresh_two,
):
    groups, _, _ = table_ref.shape
    own = 8 * 8
    half_groups = groups // 2
    half = half_groups * own
    total = jnp.zeros((1, W), F32)
    for g in range(groups):
        top = own * (g % half_groups)
        side = W * (g // half_groups)
        table_two[top : top + own, side : side + W] = table_ref[g, :own]
        tail = table_ref[g, own : own + 16].astype(F32)
        total = total + (tail[0:1] + (tail[1:2] + tail[2:3]))
    node_count = nodes_ref.shape[0]
    everyone = node_count * 8 * groups
    pooled = total / math.sqrt(everyone)
    pooled_out[...] = pooled
    region = region_ref[...]
    place = ((region >> 3) & (groups - 1)) * own + (region >> 8) * 8 + (region & 7)
    node_half = node_count // 2
    context = picked_rows(table_two[...], half, place, place.shape[0])
    context_out[...] = context
    for k in range(4):
        rows = slice(k * 256, (k + 1) * 256)
        fresh = node_update(
            0,
            nodes_ref[rows],
            summed_ref[rows],
            context[rows],
            pooled,
            w_in_ref,
            wg_ref,
            w_out_ref,
            bias_ref,
            gain_ref,
        )
        nodes_out[rows] = fresh
        top = (k * 256) % node_half
        side = W * ((k * 256) // node_half)
        fresh_two[top : top + 256, side : side + W] = fresh
    picked = send_rows(fresh_two[...], node_half, send_ref)
    for k, ref in enumerate((a_out, b_out, c_out, d_out)):
        ref[...] = picked[W * k : W * (k + 1)]


def last_node_kernel(
    layer,
    nodes_ref,
    summed_ref,
    context_ref,
    pooled_ref,
    w_in_ref,
    wg_ref,
    w_out_ref,
    bias_ref,
    gain_ref,
    nodes_out,
):
    nodes_out[...] = node_update(
        layer,
        nodes_ref[...],
        summed_ref[...],
        context_ref[...],
        pooled_ref[...],
        w_in_ref,
        wg_ref,
        w_out_ref,
        bias_ref,
        gain_ref,
    )


def exchanged(block, axis, phase):
    devices = lax.axis_size(axis)
    pairs = []
    for i in range(phase, devices - 1, 2):
        pairs += [(i, i + 1), (i + 1, i)]
    return lax.ppermute(block, axis, pairs)


def halo_of(picked):
    return [
        exchanged(picked[0], "row", 0),
        exchanged(picked[1], "row", 1),
        exchanged(picked[2], COL, 0),
        exchanged(picked[3], COL, 1),
    ]


def to_everyone(copies, axis):
    return lax.all_to_all(copies, axis, split_axis=0, concat_axis=0, tiled=True)


def local(
    node_latent,
    edge_latent,
    senders,
    receivers,
    send_index,
    context_table,
    region,
    edge_w1,
    edge_w2,
    edge_bias,
    edge_gain,
    node_w1,
    node_wg,
    node_w2,
    node_bias,
    node_gain,
):
    n_row, n_col = lax.axis_size("row"), lax.axis_size(COL)
    block = jax.ShapeDtypeStruct((W, W), BF)
    payload, *picked = pl.pallas_call(
        start_kernel,
        out_shape=[jax.ShapeDtypeStruct((n_row, 16, W), BF)] + [block] * 4,
        name="start",
    )(node_latent, send_index, context_table)
    halo = halo_of(picked)
    by_row = to_everyone(payload, "row")
    second = pl.pallas_call(
        middle_kernel,
        out_shape=jax.ShapeDtypeStruct((n_col, 80, W), BF),
        name="middle",
    )(by_row)
    table = to_everyone(second, COL)
    senders = senders.reshape(-1, W)
    receivers = receivers.reshape(-1, W)
    edges, summed = edge_step(
        0, node_latent, halo, senders, receivers, edge_latent, edge_w1, edge_w2, edge_bias, edge_gain
    )
    node_specs = [
        of_layer(node_w1.shape, 0),
        of_layer(node_wg.shape, 0),
        of_layer(node_w2.shape, 0),
        of_layer(node_bias.shape, 0),
        whole(node_gain.shape),
    ]
    node_count = node_latent.shape[0]
    region = region.reshape(-1, W)
    nodes, context, pooled, *picked = pl.pallas_call(
        first_node_kernel,
        grid=(1,),
        in_specs=[
            whole(node_latent.shape),
            whole(node_latent.shape),
            whole(table.shape),
            whole(region.shape),
            whole(send_index.shape),
            *node_specs,
        ],
        out_specs=[whole(node_latent.shape)] * 2 + [whole((1, W))] + [whole((W, W))] * 4,
        out_shape=[jax.ShapeDtypeStruct(node_latent.shape, BF)] * 2
        + [jax.ShapeDtypeStruct((1, W), F32)]
        + [block] * 4,
        scratch_shapes=[
            VM((n_col // 2 * 64, 2 * W), BF),
            VM((node_count // 2, 2 * W), BF),
        ],
        name="nodes_0",
    )(node_latent, summed, table, region, send_index, node_w1, node_wg, node_w2, node_bias, node_gain)
    halo = halo_of(picked)
    edges, summed = edge_step(
        1, nodes, halo, senders, receivers, edges, edge_w1, edge_w2, edge_bias, edge_gain
    )
    rows = 256
    strip = pl.BlockSpec((rows, W), lambda i: (i, 0))
    nodes = pl.pallas_call(
        functools.partial(last_node_kernel, 1),
        grid=(node_count // rows,),
        in_specs=[
            strip,
            strip,
            strip,
            whole((1, W)),
            of_layer(node_w1.shape, 1),
            of_layer(node_wg.shape, 1),
            of_layer(node_w2.shape, 1),
            of_layer(node_bias.shape, 1),
            whole(node_gain.shape),
        ],
        out_specs=strip,
        out_shape=jax.ShapeDtypeStruct(nodes.shape, BF),
        name="nodes_1",
    )(nodes, summed, context, pooled, node_w1, node_wg, node_w2, node_bias, node_gain)
    return (nodes, edges)


def solution(mesh):
    finer = Mesh(
        mesh.devices.reshape(mesh.shape["row"], 4, 4, 2), ("row", "col_0", "col_1", "col_2")
    )
    placed = (
        P(ROW_COL, None),
        P(ROW_COL, None),
        P(ROW_COL),
        P(ROW_COL),
        P(ROW_COL, None, None),
        P(ROW_COL, None),
        P(ROW_COL),
        P(),
        P(),
        P(),
        P(),
        P(),
        P(),
        P(),
        P(),
        P(),
    )
    return jax.shard_map(
        local,
        mesh=finer,
        in_specs=placed,
        out_specs=(P(ROW_COL, None), P(ROW_COL, None)),
        check_vma=False,
    )
```

```python
import functools
import math

import jax
import jax.numpy as jnp
from jax import lax
from jax.experimental import pallas as pl
from jax.experimental.pallas import tpu as pltpu
from jax.sharding import Mesh
from jax.sharding import PartitionSpec as P


LAYERS = 2
COL = ("col_0", "col_1", "col_2")
ROW_COL = ("row", "col_0", "col_1", "col_2")
EPS = 1e-05
W = 128
TILE = 1024
BF = jnp.bfloat16
F32 = jnp.float32
VM = pltpu.VMEM
VMEM_LIMIT = 66_600_960


def dot(a, b):
    return jnp.dot(a, b, preferred_element_type=F32)


def columns(stack, count):
    turned = jnp.transpose(stack)
    return [
        jnp.broadcast_to(turned[:, k : k + 1], (W, W)).astype(jnp.int16) for k in range(count)
    ]


def column_hot(col, count):
    lane = lax.broadcasted_iota(jnp.int16, (1, W), 1)
    one, zero = jnp.ones((), BF), jnp.zeros((), BF)
    pieces = [
        jnp.where(col == lane + jnp.int16(W * c), one, zero) for c in range(count // W)
    ]
    return jnp.concatenate(pieces, axis=1)


def row_hot(row, count):
    spread = jnp.broadcast_to(row, (16, W)).astype(jnp.int16)
    at = lax.broadcasted_iota(jnp.int16, (16, W), 0)
    one, zero = jnp.ones((), BF), jnp.zeros((), BF)
    pieces = [jnp.where(spread == at + jnp.int16(16 * c), one, zero) for c in range(count // 16)]
    return jnp.concatenate(pieces, axis=0)


def split2(value):
    high = value.astype(BF)
    low = (value - high.astype(F32)).astype(BF)
    return high, low


def split3(value):
    high = value.astype(BF)
    rest = value - high.astype(F32)
    mid = rest.astype(BF)
    low = (rest - mid.astype(F32)).astype(BF)
    return high, mid, low


def centred_weights(w_out, b_out):
    full = w_out.astype(F32)
    full = full - jnp.mean(full, axis=1, keepdims=True)
    high, low = split2(full)
    return jnp.concatenate([high, low], axis=1), b_out - jnp.mean(b_out, axis=1, keepdims=True)


def norm_tail(pre, w_two, b_centred, gain, shift):
    hidden = jnp.maximum(pre, 0.0).astype(BF)
    both = dot(hidden, w_two)
    centred = both[:, :W] + both[:, W:] + b_centred
    spread = jnp.mean(centred * centred, axis=-1, keepdims=True)
    return centred * lax.rsqrt(spread + EPS) * gain + shift


def picked_rows(table_two, half_rows, col):
    hot = column_hot(col & jnp.int16(half_rows - 1), half_rows)
    both = dot(hot, table_two)
    upper = col.astype(jnp.int32) >= half_rows
    return jnp.where(upper, both[:, W:], both[:, :W]).astype(BF)


def phases(first, second, odd):
    return jnp.where(odd, second, first), jnp.where(odd, first, second)


def start_kernel(nodes_ref, send_ref, context_ref, payload_ref, pick_col, *picked_refs):
    nodes = nodes_ref[...]
    half = nodes.shape[0] // 2
    two = jnp.concatenate([nodes[:half], nodes[half:]], axis=1)
    row_odd = lax.rem(lax.axis_index("row"), 2) == 1
    col_odd = lax.axis_index("col_2") == 1
    index = [send_ref[0, k : k + 1, :] for k in range(4)]
    index_a, index_b = phases(index[0], index[1], row_odd)
    index_c, index_d = phases(index[2], index[3], col_odd)
    stack = jnp.concatenate([index_a, index_b, index_c, index_d] + [index_a] * 4, axis=0)
    col = jnp.concatenate(columns(stack, 4), axis=0)
    pick_col[...] = col
    picked = picked_rows(two, half, col)
    for k, ref in enumerate(picked_refs):
        ref[...] = picked[W * k : W * (k + 1)]
    local_sum = jnp.sum(nodes.astype(F32), axis=0, keepdims=True)
    block = jnp.concatenate(
        [context_ref[...].astype(F32)]
        + [p.astype(F32) for p in split3(local_sum)]
        + [jnp.zeros((5, W), F32)],
        axis=0,
    ).astype(BF)
    for k in range(payload_ref.shape[0]):
        payload_ref[k] = block


def middle_kernel(got_ref, payload_ref):
    got = [got_ref[k].astype(F32) for k in range(got_ref.shape[0])]
    total = functools.reduce(
        lambda a, b: a + b, [g[8:9] + (g[9:10] + g[10:11]) for g in got]
    )
    high, mid, low = split3(total)
    block = jnp.concatenate(
        [g[:8] for g in got]
        + [high.astype(F32), mid.astype(F32), low.astype(F32), jnp.zeros((13, W), F32)],
        axis=0,
    ).astype(BF)
    for k in range(payload_ref.shape[0]):
        payload_ref[k] = block


def project(nodes, halo, w_in, send_table, recv_table):
    node_count = nodes.shape[0]
    send_half, recv_half = (node_count + 4 * W) // 2, node_count // 2
    ext = jnp.concatenate([nodes, *halo], axis=0)
    from_send = dot(ext, w_in[:W]).astype(BF)
    from_recv = dot(nodes, w_in[W : 2 * W]).astype(BF)
    send_table[:send_half, :W] = from_send[:send_half]
    send_table[:send_half, W:] = from_send[send_half:]
    send_table[send_half:, :W] = w_in[2 * W :]
    send_table[send_half:, W:] = w_in[2 * W :]
    recv_table[:, :W] = from_recv[:recv_half]
    recv_table[:, W:] = from_recv[recv_half:]


def edge_pre(edges, send16, recv16, send_table, recv_table, bias):
    recv_half = recv_table.shape[0]
    send_half = send_table.shape[0] - W
    send_local = jnp.where(send16 >= jnp.int16(send_half), send16 - jnp.int16(send_half), send16)
    send_hot = column_hot(send_local, send_half)
    recv_hot = column_hot(recv16 & jnp.int16(recv_half - 1), recv_half)
    both_s = dot(jnp.concatenate([send_hot, edges], axis=1), send_table[...])
    both_r = dot(recv_hot, recv_table[...])
    upper_s = send16.astype(jnp.int32) >= send_half
    upper_r = recv16.astype(jnp.int32) >= recv_half
    return (
        jnp.where(upper_s, both_s[:, W:], both_s[:, :W])
        + jnp.where(upper_r, both_r[:, W:], both_r[:, :W])
        + bias
    )


def edge_tail(pre, edges, recv16, recv_rows, recv_half, w_two, biases, gain):
    tail = norm_tail(pre, w_two, biases[1], gain, biases[2])
    fresh = (edges.astype(F32) + tail).astype(BF)
    lower16 = recv16 < jnp.int16(recv_half)
    zero = jnp.zeros((), BF)
    fresh_two = jnp.concatenate(
        [jnp.where(lower16, fresh, zero), jnp.where(lower16, zero, fresh)], axis=1
    )
    rows = recv_rows & (recv_half - 1)
    turned = jnp.concatenate(
        [row_hot(rows[k : k + 1], recv_half) for k in range(rows.shape[0])], axis=1
    )
    return fresh, dot(turned, fresh_two)


def edge_kernel(layer, last, *refs):
    nodes_ref, *refs = refs
    halo, refs = refs[:4], refs[4:]
    (send_hbm, recv_hbm, receivers_ref, edges_hbm, w_in_ref, w_out_ref, bias_ref, gain_ref), refs = (
        refs[:8],
        refs[8:],
    )
    if last:
        node_refs, refs = refs[:7], refs[7:]
    fresh_hbm, node_side, *refs = refs
    send_table, recv_table, acc, w_two, even_pre, odd_pre, *refs = refs
    send_col, recv_col, edges_ref, fresh_buf, in_sems, out_sems = refs
    recv_half = nodes_ref.shape[0] // 2
    steps = edges_ref.shape[0] // TILE
    per = TILE // W

    def strip(i):
        start = i * TILE
        return pl.ds(start if isinstance(i, int) else pl.multiple_of(start, TILE), TILE)

    def in_copies(i):
        at = strip(i)
        return [
            pltpu.make_async_copy(hbm.at[at], ref.at[at], in_sems.at[k, i])
            for k, (hbm, ref) in enumerate(
                ((send_hbm, send_col), (recv_hbm, recv_col), (edges_hbm, edges_ref))
            )
        ]

    def out_copy(i):
        at = strip(i)
        return pltpu.make_async_copy(fresh_buf.at[at], fresh_hbm.at[at], out_sems.at[i])

    for i in range(steps):
        for copy in in_copies(i):
            copy.start()

    project(nodes_ref[...], [h[...] for h in halo], w_in_ref[0], send_table, recv_table)
    two, b_centred = centred_weights(w_out_ref[0], bias_ref[1, layer : layer + 1])
    w_two[...] = two
    acc[...] = jnp.zeros_like(acc)
    biases = (bias_ref[0, layer : layer + 1], b_centred, bias_ref[2, layer : layer + 1])
    gain = gain_ref[layer : layer + 1]

    def arrive(i):
        for copy in in_copies(i):
            copy.wait()

    def pre_of(i):
        at = strip(i)
        return edge_pre(
            edges_ref[at], send_col[at], recv_col[at], send_table, recv_table, biases[0]
        )

    def tail_of(i, pre):
        at = strip(i)
        rows = receivers_ref[pl.ds(i * per, per)]
        return edge_tail(
            pre, edges_ref[at], recv_col[at], rows, recv_half, w_two[...], biases, gain
        )

    def both(i, now, later):
        arrive(i + 1)
        pre = pre_of(i + 1)
        fresh, added = tail_of(i, now[...])
        later[...] = pre
        acc[...] += added
        fresh_buf[strip(i)] = fresh
        out_copy(i).start()

    arrive(0)
    even_pre[...] = pre_of(0)

    def body(j, carry):
        both(2 * j, even_pre, odd_pre)
        both(2 * j + 1, odd_pre, even_pre)
        return carry

    lax.fori_loop(0, steps // 2 - 1, body, 0)
    both(steps - 2, even_pre, odd_pre)
    fresh, added = tail_of(steps - 1, odd_pre[...])
    fresh_buf[strip(steps - 1)] = fresh
    out_copy(steps - 1).start()
    sums = acc[...] + added
    summed = jnp.concatenate([sums[:, :W], sums[:, W:]], axis=0).astype(BF)
    if last:
        context_ref, pooled_ref, *weights = node_refs
        node_side[...] = node_update(
            layer, nodes_ref[...], summed, context_ref[...], pooled_ref[...], *weights
        )
    else:
        node_side[...] = summed

    def drain(i, carry):
        out_copy(i).wait()
        return carry

    lax.fori_loop(0, steps, drain, 0)


def params():
    return pltpu.CompilerParams(vmem_limit_bytes=VMEM_LIMIT)


def whole(arg):
    return pl.BlockSpec(arg.shape, lambda i: (0,) * len(arg.shape))


def of_layer(arg, layer):
    if arg.ndim != 3 or arg.shape[0] != LAYERS:
        return whole(arg)
    return pl.BlockSpec((1, *arg.shape[1:]), lambda i: (layer, 0, 0))


def edge_step(layer, last, nodes, halo, send_col, recv_col, receivers, edges, weights, node_args):
    node_count, edge_count = nodes.shape[0], edges.shape[0]
    half, ext_half = node_count // 2, (node_count + 4 * W) // 2
    flops = 2 * edge_count * W * (2 * ext_half + 4 * half + 8 * W)
    args = [nodes, *halo, send_col, recv_col, receivers, edges, *weights, *node_args]
    specs = [of_layer(arg, layer) for arg in args]
    for k in (1, 2, 3, 4):
        specs[k] = pl.BlockSpec(memory_space=VM)
    for k in (5, 6, 8):
        specs[k] = pl.BlockSpec(memory_space=pltpu.HBM)
    steps = edge_count // TILE
    return pl.pallas_call(
        functools.partial(edge_kernel, layer, last),
        grid=(1,),
        in_specs=specs,
        out_specs=[pl.BlockSpec(memory_space=pltpu.HBM), whole(nodes)],
        out_shape=[
            jax.ShapeDtypeStruct(edges.shape, BF),
            jax.ShapeDtypeStruct(nodes.shape, BF),
        ],
        scratch_shapes=[
            VM((ext_half + W, 2 * W), BF),
            VM((half, 2 * W), BF),
            VM((half, 2 * W), F32),
            VM((W, 2 * W), BF),
            VM((TILE, W), F32),
            VM((TILE, W), F32),
            VM((edge_count, W), jnp.int16),
            VM((edge_count, W), jnp.int16),
            VM(edges.shape, BF),
            VM(edges.shape, BF),
            pltpu.SemaphoreType.DMA((3, steps)),
            pltpu.SemaphoreType.DMA((steps,)),
        ],
        compiler_params=params(),
        cost_estimate=pl.CostEstimate(
            flops=flops, bytes_accessed=4 * edge_count * W, transcendentals=0
        ),
    )(*args)


def node_update(layer, nodes, summed, context, pooled, w_in_ref, wg_ref, w_out_ref, bias_ref, gain_ref):
    parts = jnp.concatenate(
        [p.astype(F32) for p in split3(pooled)] + [jnp.zeros((13, W), F32)], axis=0
    ).astype(BF)
    through = dot(parts, wg_ref[0])
    shift_in = bias_ref[0, layer : layer + 1] + (through[0:1] + (through[1:2] + through[2:3]))
    w_two, b_centred = centred_weights(w_out_ref[0], bias_ref[1, layer : layer + 1])
    feats = jnp.concatenate([nodes, summed, context], axis=1)
    pre = dot(feats, w_in_ref[0]) + shift_in
    tail = norm_tail(
        pre, w_two, b_centred, gain_ref[layer : layer + 1], bias_ref[2, layer : layer + 1]
    )
    return (nodes.astype(F32) + tail).astype(BF)


def prepare_kernel(senders_ref, receivers_ref, region_ref, send_col, recv_col, region_col):
    node_count = region_ref.shape[0] * W
    senders = senders_ref[...]
    row_flip = jnp.where(lax.rem(lax.axis_index("row"), 2) == 1, 0, W)
    col_flip = jnp.where(lax.axis_index("col_2") == 1, 0, W)
    flip = jnp.where(senders < node_count + 2 * W, row_flip, col_flip)
    senders = jnp.where(senders < node_count, senders, senders ^ flip)
    region = region_ref[...]
    place = ((region >> 3) & 31) * 64 + (region >> 8) * 8 + (region & 7)
    for values, ref in (
        (senders, send_col),
        (receivers_ref[...], recv_col),
        (place, region_col),
    ):
        for k, block in enumerate(columns(values, values.shape[0])):
            ref[W * k : W * (k + 1)] = block


def first_node_kernel(
    nodes_ref,
    summed_ref,
    table_ref,
    region_col,
    pick_col,
    w_in_ref,
    wg_ref,
    w_out_ref,
    bias_ref,
    gain_ref,
    nodes_out,
    context_out,
    pooled_out,
    a_out,
    b_out,
    c_out,
    d_out,
    table_two,
    fresh_two,
):
    groups, _, _ = table_ref.shape
    own = 8 * 8
    half_groups = groups // 2
    half = half_groups * own
    total = jnp.zeros((1, W), F32)
    for g in range(groups):
        top = own * (g % half_groups)
        side = W * (g // half_groups)
        table_two[top : top + own, side : side + W] = table_ref[g, :own]
        tail = table_ref[g, own : own + 16].astype(F32)
        total = total + (tail[0:1] + (tail[1:2] + tail[2:3]))
    node_count = nodes_ref.shape[0]
    everyone = node_count * 8 * groups
    pooled = total / math.sqrt(everyone)
    pooled_out[...] = pooled
    node_half = node_count // 2
    context = picked_rows(table_two[...], half, region_col[...])
    context_out[...] = context
    fresh = node_update(
        0,
        nodes_ref[...],
        summed_ref[...],
        context,
        pooled,
        w_in_ref,
        wg_ref,
        w_out_ref,
        bias_ref,
        gain_ref,
    )
    nodes_out[...] = fresh
    fresh_two[:, :W] = fresh[:node_half]
    fresh_two[:, W:] = fresh[node_half:]
    picked = picked_rows(fresh_two[...], node_half, pick_col[...])
    for k, ref in enumerate((a_out, b_out, c_out, d_out)):
        ref[...] = picked[W * k : W * (k + 1)]


def exchanged(block, axis, phase):
    devices = lax.axis_size(axis)
    pairs = []
    for i in range(phase, devices - 1, 2):
        pairs += [(i, i + 1), (i + 1, i)]
    return lax.ppermute(block, axis, pairs)


def halo_of(picked):
    halo = []
    for k, (axis, phase) in enumerate((("row", 0), ("row", 1), (COL, 0), (COL, 1))):
        halo.append(exchanged(picked[k], axis, phase))
    return halo


def to_everyone(copies, axis):
    return lax.all_to_all(copies, axis, split_axis=0, concat_axis=0, tiled=True)


def local(
    node_latent,
    edge_latent,
    senders,
    receivers,
    send_index,
    context_table,
    region,
    edge_w1,
    edge_w2,
    edge_bias,
    edge_gain,
    node_w1,
    node_wg,
    node_w2,
    node_bias,
    node_gain,
):
    n_row, n_col = lax.axis_size("row"), lax.axis_size(COL)
    node_count, edge_count = node_latent.shape[0], edge_latent.shape[0]
    senders, receivers, region = (v.reshape(-1, W) for v in (senders, receivers, region))
    edge_bias, node_bias = (v.transpose(1, 0, 2) for v in (edge_bias, node_bias))
    block = jax.ShapeDtypeStruct((W, W), BF)
    column = lambda rows: jax.ShapeDtypeStruct((rows, W), jnp.int16)
    payload, pick_col, *picked = pl.pallas_call(
        start_kernel,
        out_shape=[jax.ShapeDtypeStruct((n_row, 16, W), BF), column(4 * W)] + [block] * 4,
        compiler_params=params(),
        name="start",
    )(node_latent, send_index, context_table)
    by_row = to_everyone(payload, "row")
    halo = halo_of(picked)
    send_col, recv_col, region_col = pl.pallas_call(
        prepare_kernel,
        out_shape=[column(edge_count), column(edge_count), column(node_count)],
        compiler_params=params(),
        cost_estimate=pl.CostEstimate(
            flops=2 * edge_count * W * W * 4, bytes_accessed=4 * edge_count * W, transcendentals=0
        ),
        name="prepare",
    )(senders, receivers, region)
    by_row, *halo = lax.optimization_barrier((by_row, *halo))
    second = pl.pallas_call(
        middle_kernel,
        in_specs=[pl.BlockSpec(memory_space=VM)],
        out_specs=pl.BlockSpec(memory_space=VM),
        out_shape=jax.ShapeDtypeStruct((n_col, 80, W), BF),
        compiler_params=pltpu.CompilerParams(vmem_limit_bytes=8 << 20),
        name="middle",
    )(by_row)
    table = to_everyone(second, COL)
    weights = (edge_w1, edge_w2, edge_bias, edge_gain)
    node_weights = (node_w1, node_wg, node_w2, node_bias, node_gain)
    edges, summed = edge_step(
        0, False, node_latent, halo, send_col, recv_col, receivers, edge_latent, weights, ()
    )
    node_outs = (
        [jax.ShapeDtypeStruct(node_latent.shape, BF)] * 2
        + [jax.ShapeDtypeStruct((1, W), F32)]
        + [block] * 4
    )
    nodes, context, pooled, *picked = pl.pallas_call(
        first_node_kernel,
        grid=(1,),
        in_specs=[
            of_layer(v, 0) for v in (node_latent, summed, table, region_col, pick_col, *node_weights)
        ],
        out_specs=[whole(v) for v in node_outs],
        out_shape=node_outs,
        scratch_shapes=[
            VM((n_col // 2 * 64, 2 * W), BF),
            VM((node_count // 2, 2 * W), BF),
        ],
        compiler_params=params(),
        name="nodes_0",
    )(node_latent, summed, table, region_col, pick_col, *node_weights)
    halo = halo_of(picked)
    edges, nodes = edge_step(
        1,
        True,
        nodes,
        halo,
        send_col,
        recv_col,
        receivers,
        edges,
        weights,
        (context, pooled, *node_weights),
    )
    return (nodes, edges)


def solution(mesh):
    finer = Mesh(
        mesh.devices.reshape(mesh.shape["row"], 4, 4, 2), ("row", "col_0", "col_1", "col_2")
    )
    placed = (
        P(ROW_COL, None),
        P(ROW_COL, None),
        P(ROW_COL),
        P(ROW_COL),
        P(ROW_COL, None, None),
        P(ROW_COL, None),
        P(ROW_COL),
        P(),
        P(),
        P(),
        P(),
        P(),
        P(),
        P(),
        P(),
        P(),
    )
    return jax.shard_map(
        local,
        mesh=finer,
        in_specs=placed,
        out_specs=(P(ROW_COL, None), P(ROW_COL, None)),
        check_vma=False,
    )
```

```python
import functools
import math

import jax
import jax.numpy as jnp
from jax import lax
from jax.experimental import pallas as pl
from jax.experimental.pallas import tpu as pltpu
from jax.sharding import Mesh
from jax.sharding import PartitionSpec as P


LAYERS = 2
COL = ("col_0", "col_1", "col_2")
ROW_COL = ("row", "col_0", "col_1", "col_2")
EPS = 1e-05
W = 128
TILE = 1024
BF = jnp.bfloat16
F32 = jnp.float32
VM = pltpu.VMEM
VMEM_LIMIT = 66_600_960


def dot(a, b):
    return jnp.dot(a, b, preferred_element_type=F32)


def columns(stack, count):
    turned = jnp.transpose(stack)
    return [
        jnp.broadcast_to(turned[:, k : k + 1], (W, W)).astype(jnp.int16) for k in range(count)
    ]


def column_hot(col, count):
    lane = lax.broadcasted_iota(jnp.int16, (1, W), 1)
    one, zero = jnp.ones((), BF), jnp.zeros((), BF)
    pieces = [
        jnp.where(col == lane + jnp.int16(W * c), one, zero) for c in range(count // W)
    ]
    return jnp.concatenate(pieces, axis=1)


def row_hot(row, count):
    spread = jnp.broadcast_to(row, (16, W)).astype(jnp.int16)
    at = lax.broadcasted_iota(jnp.int16, (16, W), 0)
    one, zero = jnp.ones((), BF), jnp.zeros((), BF)
    pieces = [jnp.where(spread == at + jnp.int16(16 * c), one, zero) for c in range(count // 16)]
    return jnp.concatenate(pieces, axis=0)


def split2(value):
    high = value.astype(BF)
    low = (value - high.astype(F32)).astype(BF)
    return high, low


def split3(value):
    high = value.astype(BF)
    rest = value - high.astype(F32)
    mid = rest.astype(BF)
    low = (rest - mid.astype(F32)).astype(BF)
    return high, mid, low


def centred_weights(w_out, b_out):
    full = w_out.astype(F32)
    full = full - jnp.mean(full, axis=1, keepdims=True)
    high, low = split2(full)
    return jnp.concatenate([high, low], axis=1), b_out - jnp.mean(b_out, axis=1, keepdims=True)


def norm_tail(pre, w_two, b_centred, gain, shift):
    hidden = jnp.maximum(pre, 0.0).astype(BF)
    both = dot(hidden, w_two)
    centred = both[:, :W] + both[:, W:] + b_centred
    spread = jnp.mean(centred * centred, axis=-1, keepdims=True)
    return centred * lax.rsqrt(spread + EPS) * gain + shift


def picked_rows(table_two, half_rows, col):
    hot = column_hot(col & jnp.int16(half_rows - 1), half_rows)
    both = dot(hot, table_two)
    upper = col.astype(jnp.int32) >= half_rows
    return jnp.where(upper, both[:, W:], both[:, :W]).astype(BF)


def phases(first, second, odd):
    return jnp.where(odd, second, first), jnp.where(odd, first, second)


def start_kernel(nodes_ref, send_ref, context_ref, payload_ref, pick_col, *picked_refs):
    nodes = nodes_ref[...]
    half = nodes.shape[0] // 2
    two = jnp.concatenate([nodes[:half], nodes[half:]], axis=1)
    row_odd = lax.rem(lax.axis_index("row"), 2) == 1
    col_odd = lax.axis_index("col_2") == 1
    index = [send_ref[0, k : k + 1, :] for k in range(4)]
    index_a, index_b = phases(index[0], index[1], row_odd)
    index_c, index_d = phases(index[2], index[3], col_odd)
    stack = jnp.concatenate([index_a, index_b, index_c, index_d] + [index_a] * 4, axis=0)
    col = jnp.concatenate(columns(stack, 4), axis=0)
    pick_col[...] = col
    picked = picked_rows(two, half, col)
    for k, ref in enumerate(picked_refs):
        ref[...] = picked[W * k : W * (k + 1)]
    local_sum = jnp.sum(nodes.astype(F32), axis=0, keepdims=True)
    block = jnp.concatenate(
        [context_ref[...].astype(F32)]
        + [p.astype(F32) for p in split3(local_sum)]
        + [jnp.zeros((5, W), F32)],
        axis=0,
    ).astype(BF)
    for k in range(payload_ref.shape[0]):
        payload_ref[k] = block


def middle_kernel(got_ref, payload_ref):
    got = [got_ref[k].astype(F32) for k in range(got_ref.shape[0])]
    total = functools.reduce(
        lambda a, b: a + b, [g[8:9] + (g[9:10] + g[10:11]) for g in got]
    )
    high, mid, low = split3(total)
    block = jnp.concatenate(
        [g[:8] for g in got]
        + [high.astype(F32), mid.astype(F32), low.astype(F32), jnp.zeros((13, W), F32)],
        axis=0,
    ).astype(BF)
    for k in range(payload_ref.shape[0]):
        payload_ref[k] = block


def project(nodes, halo, w_in, send_table, recv_table):
    node_count = nodes.shape[0]
    send_half, recv_half = (node_count + 4 * W) // 2, node_count // 2
    ext = jnp.concatenate([nodes, *halo], axis=0)
    from_send = dot(ext, w_in[:W]).astype(BF)
    from_recv = dot(nodes, w_in[W : 2 * W]).astype(BF)
    send_table[:send_half, :W] = from_send[:send_half]
    send_table[:send_half, W:] = from_send[send_half:]
    send_table[send_half:, :W] = w_in[2 * W :]
    send_table[send_half:, W:] = w_in[2 * W :]
    recv_table[:, :W] = from_recv[:recv_half]
    recv_table[:, W:] = from_recv[recv_half:]


def edge_pre(edges, send16, recv16, send_table, recv_table, bias):
    recv_half = recv_table.shape[0]
    send_half = send_table.shape[0] - W
    send_local = jnp.where(send16 >= jnp.int16(send_half), send16 - jnp.int16(send_half), send16)
    send_hot = column_hot(send_local, send_half)
    recv_hot = column_hot(recv16 & jnp.int16(recv_half - 1), recv_half)
    both_s = dot(jnp.concatenate([send_hot, edges], axis=1), send_table[...])
    both_r = dot(recv_hot, recv_table[...])
    upper_s = send16.astype(jnp.int32) >= send_half
    upper_r = recv16.astype(jnp.int32) >= recv_half
    return (
        jnp.where(upper_s, both_s[:, W:], both_s[:, :W])
        + jnp.where(upper_r, both_r[:, W:], both_r[:, :W])
        + bias
    )


def edge_tail(pre, edges, recv16, recv_rows, recv_half, w_two, biases, gain):
    tail = norm_tail(pre, w_two, biases[1], gain, biases[2])
    fresh = (edges.astype(F32) + tail).astype(BF)
    lower16 = recv16 < jnp.int16(recv_half)
    zero = jnp.zeros((), BF)
    fresh_two = jnp.concatenate(
        [jnp.where(lower16, fresh, zero), jnp.where(lower16, zero, fresh)], axis=1
    )
    rows = recv_rows & (recv_half - 1)
    turned = jnp.concatenate(
        [row_hot(rows[k : k + 1], recv_half) for k in range(rows.shape[0])], axis=1
    )
    return fresh, dot(turned, fresh_two)


def slice_shape(arg):
    if arg.ndim != 3 or arg.shape[0] != LAYERS:
        return arg.shape
    return (1, *arg.shape[1:])


def fetches(sources, kept, sems, layer):
    copies = []
    for k, (source, ref) in enumerate(zip(sources, kept)):
        if source.shape != ref.shape:
            source = source.at[pl.ds(layer, 1)]
        copies.append(pltpu.make_async_copy(source, ref, sems.at[k]))
    return copies


def edge_kernel(layer, last, count, *refs):
    args, refs = refs[:count], refs[count:]
    send_hbm, recv_hbm, edges_hbm, *small = args
    fresh_hbm, node_side, *refs = refs
    send_table, recv_table, acc, w_two, even_pre, odd_pre, *refs = refs
    send_col, recv_col, edges_ref, fresh_buf, in_sems, out_sems, small_sems, *kept = refs
    nodes_ref, *rest = kept
    halo, rest = rest[:4], rest[4:]
    receivers_ref, w_in_ref, w_out_ref, bias_ref, gain_ref, *node_refs = rest
    early = len(kept) - len(node_refs)
    small_copies = fetches(small, kept, small_sems, layer)
    recv_half = nodes_ref.shape[0] // 2
    steps = edges_ref.shape[0] // TILE
    per = TILE // W

    def strip(i):
        start = i * TILE
        return pl.ds(start if isinstance(i, int) else pl.multiple_of(start, TILE), TILE)

    def in_copies(i):
        at = strip(i)
        return [
            pltpu.make_async_copy(hbm.at[at], ref.at[at], in_sems.at[k, i])
            for k, (hbm, ref) in enumerate(
                ((send_hbm, send_col), (recv_hbm, recv_col), (edges_hbm, edges_ref))
            )
        ]

    def out_copy(i):
        at = strip(i)
        return pltpu.make_async_copy(fresh_buf.at[at], fresh_hbm.at[at], out_sems.at[i])

    for copy in small_copies[:early] + in_copies(0):
        copy.start()
    for i in range(1, steps):
        for copy in in_copies(i):
            copy.start()
    for copy in small_copies[early:]:
        copy.start()
    for copy in small_copies[:early]:
        copy.wait()

    project(nodes_ref[...], [h[...] for h in halo], w_in_ref[0], send_table, recv_table)
    two, b_centred = centred_weights(w_out_ref[0], bias_ref[1, layer : layer + 1])
    w_two[...] = two
    acc[...] = jnp.zeros_like(acc)
    biases = (bias_ref[0, layer : layer + 1], b_centred, bias_ref[2, layer : layer + 1])
    gain = gain_ref[layer : layer + 1]

    def arrive(i):
        for copy in in_copies(i):
            copy.wait()

    def pre_of(i):
        at = strip(i)
        return edge_pre(
            edges_ref[at], send_col[at], recv_col[at], send_table, recv_table, biases[0]
        )

    def tail_of(i, pre):
        at = strip(i)
        rows = receivers_ref[pl.ds(i * per, per)]
        return edge_tail(
            pre, edges_ref[at], recv_col[at], rows, recv_half, w_two[...], biases, gain
        )

    def both(i, now, later):
        arrive(i + 1)
        fresh, added = tail_of(i, now[...])
        pre = pre_of(i + 1)
        later[...] = pre
        acc[...] += added
        fresh_buf[strip(i)] = fresh
        out_copy(i).start()

    arrive(0)
    even_pre[...] = pre_of(0)

    def body(j, carry):
        both(2 * j, even_pre, odd_pre)
        both(2 * j + 1, odd_pre, even_pre)
        return carry

    lax.fori_loop(0, steps // 2 - 1, body, 0)
    both(steps - 2, even_pre, odd_pre)
    fresh, added = tail_of(steps - 1, odd_pre[...])
    fresh_buf[strip(steps - 1)] = fresh
    out_copy(steps - 1).start()
    sums = acc[...] + added
    summed = jnp.concatenate([sums[:, :W], sums[:, W:]], axis=0).astype(BF)
    if last:
        for copy in small_copies[early:]:
            copy.wait()
        context_ref, pooled_ref, *weights = node_refs
        node_side[...] = node_update(
            layer, nodes_ref[...], summed, context_ref[...], pooled_ref[...], *weights
        )
    else:
        node_side[...] = summed

    def drain(i, carry):
        out_copy(i).wait()
        return carry

    lax.fori_loop(0, steps, drain, 0)


def params():
    return pltpu.CompilerParams(vmem_limit_bytes=VMEM_LIMIT)


def whole(arg):
    return pl.BlockSpec(arg.shape, lambda i: (0,) * len(arg.shape))


def of_layer(arg, layer):
    if arg.ndim != 3 or arg.shape[0] != LAYERS:
        return whole(arg)
    return pl.BlockSpec((1, *arg.shape[1:]), lambda i: (layer, 0, 0))


def edge_step(layer, last, nodes, halo, send_col, recv_col, receivers, edges, weights, node_args):
    node_count, edge_count = nodes.shape[0], edges.shape[0]
    half, ext_half = node_count // 2, (node_count + 4 * W) // 2
    flops = 2 * edge_count * W * (2 * ext_half + 4 * half + 8 * W)
    small = [nodes, *halo, receivers, *weights, *node_args]
    args = [send_col, recv_col, edges, *small]
    steps = edge_count // TILE
    return pl.pallas_call(
        functools.partial(edge_kernel, layer, last, len(args)),
        grid=(1,),
        in_specs=[pl.BlockSpec(memory_space=pl.ANY)] * len(args),
        out_specs=[pl.BlockSpec(memory_space=pl.ANY), whole(nodes)],
        out_shape=[
            jax.ShapeDtypeStruct(edges.shape, BF),
            jax.ShapeDtypeStruct(nodes.shape, BF),
        ],
        scratch_shapes=[
            VM((ext_half + W, 2 * W), BF),
            VM((half, 2 * W), BF),
            VM((half, 2 * W), F32),
            VM((W, 2 * W), BF),
            VM((TILE, W), F32),
            VM((TILE, W), F32),
            VM((edge_count, W), jnp.int16),
            VM((edge_count, W), jnp.int16),
            VM(edges.shape, BF),
            VM(edges.shape, BF),
            pltpu.SemaphoreType.DMA((3, steps)),
            pltpu.SemaphoreType.DMA((steps,)),
            pltpu.SemaphoreType.DMA((len(small),)),
            *[VM(slice_shape(v), v.dtype) for v in small],
        ],
        compiler_params=params(),
        cost_estimate=pl.CostEstimate(
            flops=flops, bytes_accessed=4 * edge_count * W, transcendentals=0
        ),
    )(*args)


def node_update(layer, nodes, summed, context, pooled, w_in_ref, wg_ref, w_out_ref, bias_ref, gain_ref):
    parts = jnp.concatenate(
        [p.astype(F32) for p in split3(pooled)] + [jnp.zeros((13, W), F32)], axis=0
    ).astype(BF)
    through = dot(parts, wg_ref[0])
    shift_in = bias_ref[0, layer : layer + 1] + (through[0:1] + (through[1:2] + through[2:3]))
    w_two, b_centred = centred_weights(w_out_ref[0], bias_ref[1, layer : layer + 1])
    feats = jnp.concatenate([nodes, summed, context], axis=1)
    pre = dot(feats, w_in_ref[0]) + shift_in
    tail = norm_tail(
        pre, w_two, b_centred, gain_ref[layer : layer + 1], bias_ref[2, layer : layer + 1]
    )
    return (nodes.astype(F32) + tail).astype(BF)


def prepare_kernel(senders_ref, receivers_ref, region_ref, send_col, recv_col, region_col):
    node_count = region_ref.shape[0] * W
    senders = senders_ref[...]
    row_flip = jnp.where(lax.rem(lax.axis_index("row"), 2) == 1, 0, W)
    col_flip = jnp.where(lax.axis_index("col_2") == 1, 0, W)
    flip = jnp.where(senders < node_count + 2 * W, row_flip, col_flip)
    senders = jnp.where(senders < node_count, senders, senders ^ flip)
    region = region_ref[...]
    place = ((region >> 3) & 31) * 64 + (region >> 8) * 8 + (region & 7)
    for values, ref in (
        (senders, send_col),
        (receivers_ref[...], recv_col),
        (place, region_col),
    ):
        for k, block in enumerate(columns(values, values.shape[0])):
            ref[W * k : W * (k + 1)] = block


def first_node_kernel(
    nodes_ref,
    summed_ref,
    table_ref,
    region_col,
    pick_col,
    w_in_ref,
    wg_ref,
    w_out_ref,
    bias_ref,
    gain_ref,
    nodes_out,
    context_out,
    pooled_out,
    a_out,
    b_out,
    c_out,
    d_out,
    table_two,
    fresh_two,
):
    groups, _, _ = table_ref.shape
    own = 8 * 8
    half_groups = groups // 2
    half = half_groups * own
    total = jnp.zeros((1, W), F32)
    for g in range(groups):
        top = own * (g % half_groups)
        side = W * (g // half_groups)
        table_two[top : top + own, side : side + W] = table_ref[g, :own]
        tail = table_ref[g, own : own + 16].astype(F32)
        total = total + (tail[0:1] + (tail[1:2] + tail[2:3]))
    node_count = nodes_ref.shape[0]
    everyone = node_count * 8 * groups
    pooled = total / math.sqrt(everyone)
    pooled_out[...] = pooled
    node_half = node_count // 2
    context = picked_rows(table_two[...], half, region_col[...])
    context_out[...] = context
    fresh = node_update(
        0,
        nodes_ref[...],
        summed_ref[...],
        context,
        pooled,
        w_in_ref,
        wg_ref,
        w_out_ref,
        bias_ref,
        gain_ref,
    )
    nodes_out[...] = fresh
    fresh_two[:, :W] = fresh[:node_half]
    fresh_two[:, W:] = fresh[node_half:]
    picked = picked_rows(fresh_two[...], node_half, pick_col[...])
    for k, ref in enumerate((a_out, b_out, c_out, d_out)):
        ref[...] = picked[W * k : W * (k + 1)]


def exchanged(block, axis, phase):
    devices = lax.axis_size(axis)
    pairs = []
    for i in range(phase, devices - 1, 2):
        pairs += [(i, i + 1), (i + 1, i)]
    return lax.ppermute(block, axis, pairs)


def halo_of(picked):
    halo = []
    for k, (axis, phase) in enumerate((("row", 0), ("row", 1), (COL, 0), (COL, 1))):
        halo.append(exchanged(picked[k], axis, phase))
    return halo


def to_everyone(copies, axis):
    return lax.all_to_all(copies, axis, split_axis=0, concat_axis=0, tiled=True)


def local(
    node_latent,
    edge_latent,
    senders,
    receivers,
    send_index,
    context_table,
    region,
    edge_w1,
    edge_w2,
    edge_bias,
    edge_gain,
    node_w1,
    node_wg,
    node_w2,
    node_bias,
    node_gain,
):
    n_row, n_col = lax.axis_size("row"), lax.axis_size(COL)
    node_count, edge_count = node_latent.shape[0], edge_latent.shape[0]
    senders, receivers, region = (v.reshape(-1, W) for v in (senders, receivers, region))
    edge_bias, node_bias = (v.transpose(1, 0, 2) for v in (edge_bias, node_bias))
    block = jax.ShapeDtypeStruct((W, W), BF)
    column = lambda rows: jax.ShapeDtypeStruct((rows, W), jnp.int16)
    payload, pick_col, *picked = pl.pallas_call(
        start_kernel,
        out_shape=[jax.ShapeDtypeStruct((n_row, 16, W), BF), column(4 * W)] + [block] * 4,
        compiler_params=params(),
        name="start",
    )(node_latent, send_index, context_table)
    by_row = to_everyone(payload, "row")
    halo = halo_of(picked)
    send_col, recv_col, region_col = pl.pallas_call(
        prepare_kernel,
        out_shape=[column(edge_count), column(edge_count), column(node_count)],
        compiler_params=params(),
        cost_estimate=pl.CostEstimate(
            flops=2 * edge_count * W * W * 4, bytes_accessed=4 * edge_count * W, transcendentals=0
        ),
        name="prepare",
    )(senders, receivers, region)
    by_row, *halo = lax.optimization_barrier((by_row, *halo))
    second = pl.pallas_call(
        middle_kernel,
        in_specs=[pl.BlockSpec(memory_space=VM)],
        out_specs=pl.BlockSpec(memory_space=VM),
        out_shape=jax.ShapeDtypeStruct((n_col, 80, W), BF),
        compiler_params=pltpu.CompilerParams(vmem_limit_bytes=8 << 20),
        name="middle",
    )(by_row)
    table = to_everyone(second, COL)
    weights = (edge_w1, edge_w2, edge_bias, edge_gain)
    node_weights = (node_w1, node_wg, node_w2, node_bias, node_gain)
    edges, summed = edge_step(
        0, False, node_latent, halo, send_col, recv_col, receivers, edge_latent, weights, ()
    )
    node_outs = (
        [jax.ShapeDtypeStruct(node_latent.shape, BF)] * 2
        + [jax.ShapeDtypeStruct((1, W), F32)]
        + [block] * 4
    )
    nodes, context, pooled, *picked = pl.pallas_call(
        first_node_kernel,
        grid=(1,),
        in_specs=[
            of_layer(v, 0) for v in (node_latent, summed, table, region_col, pick_col, *node_weights)
        ],
        out_specs=[whole(v) for v in node_outs],
        out_shape=node_outs,
        scratch_shapes=[
            VM((n_col // 2 * 64, 2 * W), BF),
            VM((node_count // 2, 2 * W), BF),
        ],
        compiler_params=params(),
        name="nodes_0",
    )(node_latent, summed, table, region_col, pick_col, *node_weights)
    halo = halo_of(picked)
    edges, nodes = edge_step(
        1,
        True,
        nodes,
        halo,
        send_col,
        recv_col,
        receivers,
        edges,
        weights,
        (context, pooled, *node_weights),
    )
    return (nodes, edges)


def solution(mesh):
    finer = Mesh(
        mesh.devices.reshape(mesh.shape["row"], 4, 4, 2), ("row", "col_0", "col_1", "col_2")
    )
    placed = (
        P(ROW_COL, None),
        P(ROW_COL, None),
        P(ROW_COL),
        P(ROW_COL),
        P(ROW_COL, None, None),
        P(ROW_COL, None),
        P(ROW_COL),
        P(),
        P(),
        P(),
        P(),
        P(),
        P(),
        P(),
        P(),
        P(),
    )
    return jax.shard_map(
        local,
        mesh=finer,
        in_specs=placed,
        out_specs=(P(ROW_COL, None), P(ROW_COL, None)),
        check_vma=False,
    )
```

```python
import functools
import math

import jax
import jax.numpy as jnp
from jax import lax
from jax.experimental import pallas as pl
from jax.experimental.pallas import tpu as pltpu
from jax.sharding import Mesh
from jax.sharding import PartitionSpec as P


LAYERS = 2
COL = ("col_0", "col_1", "col_2")
ROW_COL = ("row", "col_0", "col_1", "col_2")
EPS = 1e-05
W = 128
TILE = 1024
SEND_BITS = 11
BF = jnp.bfloat16
F32 = jnp.float32
VM = pltpu.VMEM
VMEM_LIMIT = 66_600_960


def dot(a, b):
    return jnp.dot(a, b, preferred_element_type=F32)


def columns(stack, count):
    turned = jnp.transpose(stack)
    return [
        jnp.broadcast_to(turned[:, k : k + 1], (W, W)).astype(jnp.int16) for k in range(count)
    ]


def column_hot(col, count):
    lane = lax.broadcasted_iota(jnp.int16, (1, W), 1)
    one, zero = jnp.ones((), BF), jnp.zeros((), BF)
    pieces = [
        jnp.where(col == lane + jnp.int16(W * c), one, zero) for c in range(count // W)
    ]
    return jnp.concatenate(pieces, axis=1)


def row_hot(row, count):
    spread = jnp.broadcast_to(row, (16, W)).astype(jnp.int16)
    at = lax.broadcasted_iota(jnp.int16, (16, W), 0)
    one, zero = jnp.ones((), BF), jnp.zeros((), BF)
    pieces = [jnp.where(spread == at + jnp.int16(16 * c), one, zero) for c in range(count // 16)]
    return jnp.concatenate(pieces, axis=0)


def split2(value):
    high = value.astype(BF)
    low = (value - high.astype(F32)).astype(BF)
    return high, low


def split3(value):
    high = value.astype(BF)
    rest = value - high.astype(F32)
    mid = rest.astype(BF)
    low = (rest - mid.astype(F32)).astype(BF)
    return high, mid, low


def centred_weights(w_out, b_out):
    full = w_out.astype(F32)
    full = full - jnp.mean(full, axis=1, keepdims=True)
    high, low = split2(full)
    return jnp.concatenate([high, low], axis=1), b_out - jnp.mean(b_out, axis=1, keepdims=True)


def norm_tail(pre, w_two, b_centred, gain, shift):
    hidden = jnp.maximum(pre, 0.0).astype(BF)
    both = dot(hidden, w_two)
    centred = both[:, :W] + both[:, W:] + b_centred
    spread = jnp.mean(centred * centred, axis=-1, keepdims=True)
    return centred * lax.rsqrt(spread + EPS) * gain + shift


def picked_rows(table_two, half_rows, col):
    hot = column_hot(col & jnp.int16(half_rows - 1), half_rows)
    both = dot(hot, table_two)
    upper = col.astype(jnp.int32) >= half_rows
    return jnp.where(upper, both[:, W:], both[:, :W]).astype(BF)


def phases(first, second, odd):
    return jnp.where(odd, second, first), jnp.where(odd, first, second)


def start_kernel(nodes_ref, send_ref, context_ref, payload_ref, pick_col, *picked_refs):
    nodes = nodes_ref[...]
    half = nodes.shape[0] // 2
    two = jnp.concatenate([nodes[:half], nodes[half:]], axis=1)
    row_odd = lax.rem(lax.axis_index("row"), 2) == 1
    col_odd = lax.axis_index("col_2") == 1
    index = [send_ref[0, k : k + 1, :] for k in range(4)]
    index_a, index_b = phases(index[0], index[1], row_odd)
    index_c, index_d = phases(index[2], index[3], col_odd)
    stack = jnp.concatenate([index_a, index_b, index_c, index_d] + [index_a] * 4, axis=0)
    col = jnp.concatenate(columns(stack, 4), axis=0)
    pick_col[...] = col
    picked = picked_rows(two, half, col)
    for k, ref in enumerate(picked_refs):
        ref[...] = picked[W * k : W * (k + 1)]
    local_sum = jnp.sum(nodes.astype(F32), axis=0, keepdims=True)
    block = jnp.concatenate(
        [context_ref[...].astype(F32)]
        + [p.astype(F32) for p in split3(local_sum)]
        + [jnp.zeros((5, W), F32)],
        axis=0,
    ).astype(BF)
    for k in range(payload_ref.shape[0]):
        payload_ref[k] = block


def middle_kernel(got_ref, payload_ref):
    got = [got_ref[k].astype(F32) for k in range(got_ref.shape[0])]
    total = functools.reduce(
        lambda a, b: a + b, [g[8:9] + (g[9:10] + g[10:11]) for g in got]
    )
    high, mid, low = split3(total)
    block = jnp.concatenate(
        [g[:8] for g in got]
        + [high.astype(F32), mid.astype(F32), low.astype(F32), jnp.zeros((13, W), F32)],
        axis=0,
    ).astype(BF)
    for k in range(payload_ref.shape[0]):
        payload_ref[k] = block


def project(nodes, halo, w_in, send_table, recv_table):
    node_count = nodes.shape[0]
    send_half, recv_half = (node_count + 4 * W) // 2, node_count // 2
    ext = jnp.concatenate([nodes, *halo], axis=0)
    from_send = dot(ext, w_in[:W]).astype(BF)
    from_recv = dot(nodes, w_in[W : 2 * W]).astype(BF)
    send_table[:send_half, :W] = from_send[:send_half]
    send_table[:send_half, W:] = from_send[send_half:]
    send_table[send_half:, :W] = w_in[2 * W :]
    send_table[send_half:, W:] = w_in[2 * W :]
    recv_table[:, :W] = from_recv[:recv_half]
    recv_table[:, W:] = from_recv[recv_half:]


def edge_pre(edges, send16, recv16, send_table, recv_table, bias):
    recv_half = recv_table.shape[0]
    send_half = send_table.shape[0] - W
    send_local = jnp.where(send16 >= jnp.int16(send_half), send16 - jnp.int16(send_half), send16)
    send_hot = column_hot(send_local, send_half)
    recv_hot = column_hot(recv16 & jnp.int16(recv_half - 1), recv_half)
    both_s = dot(jnp.concatenate([send_hot, edges], axis=1), send_table[...])
    both_r = dot(recv_hot, recv_table[...])
    upper_s = send16.astype(jnp.int32) >= send_half
    upper_r = recv16.astype(jnp.int32) >= recv_half
    return (
        jnp.where(upper_s, both_s[:, W:], both_s[:, :W])
        + jnp.where(upper_r, both_r[:, W:], both_r[:, :W])
        + bias
    )


def edge_tail(pre, edges, recv16, recv_rows, recv_half, w_two, biases, gain):
    tail = norm_tail(pre, w_two, biases[1], gain, biases[2])
    fresh = (edges.astype(F32) + tail).astype(BF)
    lower16 = recv16 < jnp.int16(recv_half)
    zero = jnp.zeros((), BF)
    fresh_two = jnp.concatenate(
        [jnp.where(lower16, fresh, zero), jnp.where(lower16, zero, fresh)], axis=1
    )
    rows = recv_rows & (recv_half - 1)
    turned = jnp.concatenate(
        [row_hot(rows[k : k + 1], recv_half) for k in range(rows.shape[0])], axis=1
    )
    return fresh, dot(turned, fresh_two)


def slice_shape(arg):
    if arg.ndim != 3 or arg.shape[0] != LAYERS:
        return arg.shape
    return (1, *arg.shape[1:])


def fetches(sources, kept, sems, layer):
    copies = []
    for k, (source, ref) in enumerate(zip(sources, kept)):
        if source.shape != ref.shape:
            source = source.at[pl.ds(layer, 1)]
        copies.append(pltpu.make_async_copy(source, ref, sems.at[k]))
    return copies


def edge_kernel(layer, last, count, *refs):
    args, refs = refs[:count], refs[count:]
    send_hbm, recv_hbm, edges_hbm, *small = args
    fresh_hbm, node_side, *refs = refs
    send_table, recv_table, acc, w_two, even_pre, odd_pre, *refs = refs
    send_col, recv_col, edges_ref, fresh_buf, in_sems, out_sems, small_sems, *kept = refs
    nodes_ref, *rest = kept
    halo, rest = rest[:4], rest[4:]
    receivers_ref, w_in_ref, w_out_ref, bias_ref, gain_ref, *node_refs = rest
    early = len(kept) - len(node_refs)
    small_copies = fetches(small, kept, small_sems, layer)
    recv_half = nodes_ref.shape[0] // 2
    steps = edges_ref.shape[0] // TILE
    per = TILE // W

    def strip(i):
        start = i * TILE
        return pl.ds(start if isinstance(i, int) else pl.multiple_of(start, TILE), TILE)

    def in_copies(i):
        at = strip(i)
        return [
            pltpu.make_async_copy(hbm.at[at], ref.at[at], in_sems.at[k, i])
            for k, (hbm, ref) in enumerate(
                ((send_hbm, send_col), (recv_hbm, recv_col), (edges_hbm, edges_ref))
            )
        ]

    def out_copy(i):
        at = strip(i)
        return pltpu.make_async_copy(fresh_buf.at[at], fresh_hbm.at[at], out_sems.at[i])

    for copy in small_copies[:early] + in_copies(0):
        copy.start()
    for i in range(1, steps):
        for copy in in_copies(i):
            copy.start()
    for copy in small_copies[early:]:
        copy.start()
    for copy in small_copies[:early]:
        copy.wait()

    project(nodes_ref[...], [h[...] for h in halo], w_in_ref[0], send_table, recv_table)
    two, b_centred = centred_weights(w_out_ref[0], bias_ref[1, layer : layer + 1])
    w_two[...] = two
    acc[...] = jnp.zeros_like(acc)
    biases = (bias_ref[0, layer : layer + 1], b_centred, bias_ref[2, layer : layer + 1])
    gain = gain_ref[layer : layer + 1]

    def arrive(i):
        for copy in in_copies(i):
            copy.wait()

    def pre_of(i):
        at = strip(i)
        return edge_pre(
            edges_ref[at], send_col[at], recv_col[at], send_table, recv_table, biases[0]
        )

    def tail_of(i, pre):
        at = strip(i)
        rows = receivers_ref[pl.ds(i * per, per)]
        return edge_tail(
            pre, edges_ref[at], recv_col[at], rows, recv_half, w_two[...], biases, gain
        )

    def both(i, now, later):
        arrive(i + 1)
        fresh, added = tail_of(i, now[...])
        pre = pre_of(i + 1)
        later[...] = pre
        acc[...] += added
        fresh_buf[strip(i)] = fresh
        out_copy(i).start()

    arrive(0)
    even_pre[...] = pre_of(0)

    def body(j, carry):
        both(2 * j, even_pre, odd_pre)
        both(2 * j + 1, odd_pre, even_pre)
        return carry

    lax.fori_loop(0, steps // 2 - 1, body, 0)
    both(steps - 2, even_pre, odd_pre)
    fresh, added = tail_of(steps - 1, odd_pre[...])
    fresh_buf[strip(steps - 1)] = fresh
    out_copy(steps - 1).start()
    sums = acc[...] + added
    summed = jnp.concatenate([sums[:, :W], sums[:, W:]], axis=0).astype(BF)
    if last:
        for copy in small_copies[early:]:
            copy.wait()
        context_ref, pooled_ref, *weights = node_refs
        node_side[...] = node_update(
            layer, nodes_ref[...], summed, context_ref[...], pooled_ref[...], *weights
        )
    else:
        node_side[...] = summed

    def drain(i, carry):
        out_copy(i).wait()
        return carry

    lax.fori_loop(0, steps, drain, 0)


def params():
    return pltpu.CompilerParams(vmem_limit_bytes=VMEM_LIMIT)


def whole(arg):
    return pl.BlockSpec(arg.shape, lambda i: (0,) * len(arg.shape))


def of_layer(arg, layer):
    if arg.ndim != 3 or arg.shape[0] != LAYERS:
        return whole(arg)
    return pl.BlockSpec((1, *arg.shape[1:]), lambda i: (layer, 0, 0))


def edge_step(layer, last, nodes, halo, send_col, recv_col, receivers, edges, weights, node_args):
    node_count, edge_count = nodes.shape[0], edges.shape[0]
    half, ext_half = node_count // 2, (node_count + 4 * W) // 2
    flops = 2 * edge_count * W * (2 * ext_half + 4 * half + 8 * W)
    small = [nodes, *halo, receivers, *weights, *node_args]
    args = [send_col, recv_col, edges, *small]
    steps = edge_count // TILE
    return pl.pallas_call(
        functools.partial(edge_kernel, layer, last, len(args)),
        grid=(1,),
        in_specs=[pl.BlockSpec(memory_space=pl.ANY)] * len(args),
        out_specs=[pl.BlockSpec(memory_space=pl.ANY), whole(nodes)],
        out_shape=[
            jax.ShapeDtypeStruct(edges.shape, BF),
            jax.ShapeDtypeStruct(nodes.shape, BF),
        ],
        scratch_shapes=[
            VM((ext_half + W, 2 * W), BF),
            VM((half, 2 * W), BF),
            VM((half, 2 * W), F32),
            VM((W, 2 * W), BF),
            VM((TILE, W), F32),
            VM((TILE, W), F32),
            VM((edge_count, W), jnp.int16),
            VM((edge_count, W), jnp.int16),
            VM(edges.shape, BF),
            VM(edges.shape, BF),
            pltpu.SemaphoreType.DMA((3, steps)),
            pltpu.SemaphoreType.DMA((steps,)),
            pltpu.SemaphoreType.DMA((len(small),)),
            *[VM(slice_shape(v), v.dtype) for v in small],
        ],
        compiler_params=params(),
        cost_estimate=pl.CostEstimate(
            flops=flops, bytes_accessed=4 * edge_count * W, transcendentals=0
        ),
    )(*args)


def node_update(layer, nodes, summed, context, pooled, w_in_ref, wg_ref, w_out_ref, bias_ref, gain_ref):
    parts = jnp.concatenate(
        [p.astype(F32) for p in split3(pooled)] + [jnp.zeros((13, W), F32)], axis=0
    ).astype(BF)
    through = dot(parts, wg_ref[0])
    shift_in = bias_ref[0, layer : layer + 1] + (through[0:1] + (through[1:2] + through[2:3]))
    w_two, b_centred = centred_weights(w_out_ref[0], bias_ref[1, layer : layer + 1])
    feats = jnp.concatenate([nodes, summed, context], axis=1)
    pre = dot(feats, w_in_ref[0]) + shift_in
    tail = norm_tail(
        pre, w_two, b_centred, gain_ref[layer : layer + 1], bias_ref[2, layer : layer + 1]
    )
    return (nodes.astype(F32) + tail).astype(BF)


def prepare_kernel(senders_ref, receivers_ref, region_ref, send_col, recv_col, region_col):
    node_count = region_ref.shape[0] * W
    senders = senders_ref[...]
    row_flip = jnp.where(lax.rem(lax.axis_index("row"), 2) == 1, 0, W)
    col_flip = jnp.where(lax.axis_index("col_2") == 1, 0, W)
    flip = jnp.where(senders < node_count + 2 * W, row_flip, col_flip)
    senders = jnp.where(senders < node_count, senders, senders ^ flip)
    region = region_ref[...]
    place = ((region >> 3) & 31) * 64 + (region >> 8) * 8 + (region & 7)
    both = jnp.transpose((receivers_ref[...] << SEND_BITS) | senders)
    for k in range(both.shape[1]):
        wide = jnp.broadcast_to(both[:, k : k + 1], (W, W))
        rows = slice(W * k, W * (k + 1))
        send_col[rows] = (wide & (2**SEND_BITS - 1)).astype(jnp.int16)
        recv_col[rows] = (wide >> SEND_BITS).astype(jnp.int16)
    for k, block in enumerate(columns(place, place.shape[0])):
        region_col[W * k : W * (k + 1)] = block


def first_node_kernel(
    nodes_ref,
    summed_ref,
    table_ref,
    region_col,
    pick_col,
    w_in_ref,
    wg_ref,
    w_out_ref,
    bias_ref,
    gain_ref,
    nodes_out,
    context_out,
    pooled_out,
    a_out,
    b_out,
    c_out,
    d_out,
    table_two,
    fresh_two,
):
    groups, _, _ = table_ref.shape
    own = 8 * 8
    half_groups = groups // 2
    half = half_groups * own
    total = jnp.zeros((1, W), F32)
    for g in range(groups):
        top = own * (g % half_groups)
        side = W * (g // half_groups)
        table_two[top : top + own, side : side + W] = table_ref[g, :own]
        tail = table_ref[g, own : own + 16].astype(F32)
        total = total + (tail[0:1] + (tail[1:2] + tail[2:3]))
    node_count = nodes_ref.shape[0]
    everyone = node_count * 8 * groups
    pooled = total / math.sqrt(everyone)
    pooled_out[...] = pooled
    node_half = node_count // 2
    context = picked_rows(table_two[...], half, region_col[...])
    context_out[...] = context
    fresh = node_update(
        0,
        nodes_ref[...],
        summed_ref[...],
        context,
        pooled,
        w_in_ref,
        wg_ref,
        w_out_ref,
        bias_ref,
        gain_ref,
    )
    nodes_out[...] = fresh
    fresh_two[:, :W] = fresh[:node_half]
    fresh_two[:, W:] = fresh[node_half:]
    picked = picked_rows(fresh_two[...], node_half, pick_col[...])
    for k, ref in enumerate((a_out, b_out, c_out, d_out)):
        ref[...] = picked[W * k : W * (k + 1)]


def exchanged(block, axis, phase):
    devices = lax.axis_size(axis)
    pairs = []
    for i in range(phase, devices - 1, 2):
        pairs += [(i, i + 1), (i + 1, i)]
    return lax.ppermute(block, axis, pairs)


def halo_of(picked):
    halo = []
    for k, (axis, phase) in enumerate((("row", 0), ("row", 1), (COL, 0), (COL, 1))):
        halo.append(exchanged(picked[k], axis, phase))
    return halo


def to_everyone(copies, axis):
    return lax.all_to_all(copies, axis, split_axis=0, concat_axis=0, tiled=True)


def local(
    node_latent,
    edge_latent,
    senders,
    receivers,
    send_index,
    context_table,
    region,
    edge_w1,
    edge_w2,
    edge_bias,
    edge_gain,
    node_w1,
    node_wg,
    node_w2,
    node_bias,
    node_gain,
):
    n_row, n_col = lax.axis_size("row"), lax.axis_size(COL)
    node_count, edge_count = node_latent.shape[0], edge_latent.shape[0]
    senders, receivers, region = (v.reshape(-1, W) for v in (senders, receivers, region))
    edge_bias, node_bias = (v.transpose(1, 0, 2) for v in (edge_bias, node_bias))
    block = jax.ShapeDtypeStruct((W, W), BF)
    column = lambda rows: jax.ShapeDtypeStruct((rows, W), jnp.int16)
    payload, pick_col, *picked = pl.pallas_call(
        start_kernel,
        out_shape=[jax.ShapeDtypeStruct((n_row, 16, W), BF), column(4 * W)] + [block] * 4,
        compiler_params=params(),
        name="start",
    )(node_latent, send_index, context_table)
    by_row = to_everyone(payload, "row")
    halo = halo_of(picked)
    send_col, recv_col, region_col = pl.pallas_call(
        prepare_kernel,
        out_shape=[column(edge_count), column(edge_count), column(node_count)],
        compiler_params=params(),
        cost_estimate=pl.CostEstimate(
            flops=2 * edge_count * W * W * 4, bytes_accessed=4 * edge_count * W, transcendentals=0
        ),
        name="prepare",
    )(senders, receivers, region)
    by_row, *halo = lax.optimization_barrier((by_row, *halo))
    second = pl.pallas_call(
        middle_kernel,
        in_specs=[pl.BlockSpec(memory_space=VM)],
        out_specs=pl.BlockSpec(memory_space=VM),
        out_shape=jax.ShapeDtypeStruct((n_col, 80, W), BF),
        compiler_params=pltpu.CompilerParams(vmem_limit_bytes=8 << 20),
        name="middle",
    )(by_row)
    table = to_everyone(second, COL)
    weights = (edge_w1, edge_w2, edge_bias, edge_gain)
    node_weights = (node_w1, node_wg, node_w2, node_bias, node_gain)
    edges, summed = edge_step(
        0, False, node_latent, halo, send_col, recv_col, receivers, edge_latent, weights, ()
    )
    node_outs = (
        [jax.ShapeDtypeStruct(node_latent.shape, BF)] * 2
        + [jax.ShapeDtypeStruct((1, W), F32)]
        + [block] * 4
    )
    nodes, context, pooled, *picked = pl.pallas_call(
        first_node_kernel,
        grid=(1,),
        in_specs=[
            of_layer(v, 0) for v in (node_latent, summed, table, region_col, pick_col, *node_weights)
        ],
        out_specs=[whole(v) for v in node_outs],
        out_shape=node_outs,
        scratch_shapes=[
            VM((n_col // 2 * 64, 2 * W), BF),
            VM((node_count // 2, 2 * W), BF),
        ],
        compiler_params=params(),
        name="nodes_0",
    )(node_latent, summed, table, region_col, pick_col, *node_weights)
    halo = halo_of(picked)
    edges, nodes = edge_step(
        1,
        True,
        nodes,
        halo,
        send_col,
        recv_col,
        receivers,
        edges,
        weights,
        (context, pooled, *node_weights),
    )
    return (nodes, edges)


def solution(mesh):
    finer = Mesh(
        mesh.devices.reshape(mesh.shape["row"], 4, 4, 2), ("row", "col_0", "col_1", "col_2")
    )
    placed = (
        P(ROW_COL, None),
        P(ROW_COL, None),
        P(ROW_COL),
        P(ROW_COL),
        P(ROW_COL, None, None),
        P(ROW_COL, None),
        P(ROW_COL),
        P(),
        P(),
        P(),
        P(),
        P(),
        P(),
        P(),
        P(),
        P(),
    )
    return jax.shard_map(
        local,
        mesh=finer,
        in_specs=placed,
        out_specs=(P(ROW_COL, None), P(ROW_COL, None)),
        check_vma=False,
    )
```
